32 devices in a mesh: band: 8 (over y, x, core), ga: 4 (over z).
Axes of the slice: x: 2, y: 2, z: 4, core: 2. Of those that a mesh axis runs over, the one named last changes fastest.
Arguments:
- orbitals: bfloat16 [256, 90112], P(('band', 'ga')), may hold values from -6 to 6
- local_part: bfloat16 [256, 90112], P(('band', 'ga')), may hold values from -6 to 6
- projectors: bfloat16 [90112, 1664], P(('band', 'ga')), may hold values from -0.01953125 to 0.01953125
- couplings: float32 [4, 13, 13], replicated, may hold values from -20 to 20, as said below
- species: int32 [128], replicated, may hold values from 0 to 3
Outputs:
- applied: bfloat16 [256, 90112], P(('band', 'ga'))
The draws below stay inside these ranges and needn't reach their ends.
Inputs may be any that keep to these rules, and one draw needn't show every extreme that they name: `couplings`: each species has one symmetric block.
All inputs are finite; a program needn't handle non-finite values.
Results may differ from the reference program's by a relative error of at most 0.0056.
Values may be sent and summed in bfloat16 or wider, within the bound.
A program may use at most 64 MiB of HBM per device.

```python
import math
import jax
import jax.numpy as jnp
from jax import lax

GVEC = 90112
PROJ = 13
SPECIES = 4
ATOMS = 128
BANDS = 256


def draw_couplings(key, part):
    first, second, third = jax.random.split(jax.random.fold_in(key, 11), 3)
    magnitude = jnp.exp(jax.random.uniform(first, (SPECIES, PROJ), minval=math.log(4.0), maxval=math.log(16.0)))
    signs = jnp.where(jax.random.bernoulli(second, 0.5, (SPECIES, PROJ)), 1.0, -1.0)
    offdiag = jnp.clip(jax.random.normal(third, (SPECIES, PROJ, PROJ)) * 0.5, -3.0, 3.0)
    offdiag = (offdiag + jnp.swapaxes(offdiag, 1, 2)) * 0.7071
    identity = jnp.eye(PROJ, dtype=jnp.float32)
    return (offdiag * (1.0 - identity) + identity[None] * (signs * magnitude)[:, :, None]).astype(jnp.float32)


def place_ends(entries, key, low, high):
    index_at = [jax.random.randint(jax.random.fold_in(key, axis), (), 0, length) for axis, length in enumerate(entries.shape)]
    main_axis = entries.shape.index(max(entries.shape))
    neighbour = index_at[:main_axis] + [(index_at[main_axis] + 1) % entries.shape[main_axis]] + index_at[main_axis + 1:]
    return entries.at[tuple(index_at)].set(low).at[tuple(neighbour)].set(high)


def spiked(entries, key, source, target, parts, factor):
    owner, partner = [(jnp.arange(entries.shape[dim]) // (entries.shape[dim] // parts)).reshape([-1 if axis == dim else 1 for axis in range(entries.ndim)]) for dim in (source, target)]
    chosen = jax.random.permutation(key, parts)[partner]
    strong = (owner == chosen) | (owner == (partner + parts // 2) % parts)
    return jnp.where(strong, factor * entries, entries)


def shard_levels(stream_key, dims, shards, smallest, top_value):
    def one(axis_at, parts):
        draws = jax.random.uniform(jax.random.fold_in(jax.random.fold_in(stream_key, 6), axis_at), (parts,), jnp.float32, smallest / len(shards), top_value / len(shards))
        return jnp.repeat(jnp.exp(draws), dims[axis_at] // parts).reshape((-1,) + (1,) * (len(dims) - axis_at - 1))

    loudness = one(*shards[0])
    for cut in shards[1:]:
        loudness = loudness * one(*cut)
    return loudness


def normal_values(rng, dims, scale, most, pieces=(), held_as=jnp.bfloat16):
    entries = jax.random.normal(rng, dims, jnp.float32) * scale
    if len(pieces) > 0:
        entries = shard_levels(rng, dims, pieces, -0.22, 0.18) * entries
    return jnp.clip(entries, min=-most, max=most).astype(held_as)


def bell_draw_with(rng, extent, deviation, most, pieces, heavy, held_as=jnp.bfloat16):
    result = deviation * jax.random.normal(rng, extent, jnp.float32)
    if pieces:
        result = result * shard_levels(rng, extent, pieces, -0.22, 0.18)
    return jnp.clip(spiked(result, jax.random.fold_in(rng, 3), *heavy), -most, most).astype(held_as)


def setup_inputs(seed: int = 0) -> dict:
    key_list = jax.random.split(jax.random.key(seed), 6)
    orbitals = bell_draw_with(key_list[0], (BANDS, GVEC), 1.0, 6.0, ((0, 32),), (1, 0, 32, 2.75))
    local_part = normal_values(key_list[1], (BANDS, GVEC), 1.0, 6.0, ((0, 32),))
    projectors = normal_values(key_list[2], (GVEC, PROJ * ATOMS), GVEC ** -0.5, 0.01953125, ((0, 32),))
    couplings = draw_couplings(jax.random.fold_in(key_list[5], 71), 0)
    species = place_ends(jax.random.randint(key_list[4], (ATOMS,), 0, SPECIES), jax.random.fold_in(key_list[4], 1), 0, SPECIES - 1).astype(jnp.int32)
    return {"orbitals": orbitals, "local_part": local_part, "projectors": projectors, "couplings": couplings, "species": species}


def reference(orbitals, local_part, projectors, couplings, species):
    select = (species[:, None] == jnp.arange(SPECIES, dtype=jnp.int32)[None, :]).astype(jnp.float32)
    blocks = jnp.dot(select, couplings.reshape(SPECIES, PROJ * PROJ), precision=lax.Precision.HIGHEST)
    blocks = blocks.reshape(ATOMS, PROJ, PROJ)
    totals = jnp.dot(orbitals, projectors, preferred_element_type=jnp.float32)
    folded = totals.reshape(BANDS, PROJ, ATOMS)
    mixed = jnp.einsum("bia,aij->bja", folded, blocks, precision=lax.Precision.HIGHEST)
    coefs = mixed.reshape(BANDS, PROJ * ATOMS).astype(jnp.bfloat16)
    correction = jnp.dot(coefs, projectors.T, preferred_element_type=jnp.float32).astype(jnp.bfloat16)
    correction = lax.optimization_barrier(correction)
    return (local_part.astype(jnp.float32) + correction.astype(jnp.float32)).astype(jnp.bfloat16)
```

```python
import jax
import jax.numpy as jnp
from jax import lax
from jax.sharding import PartitionSpec as P


def select_blocks(couplings, species):
    kinds = couplings.shape[0]
    width = couplings.shape[1]
    select = (jnp.arange(kinds, dtype=jnp.int32)[:, None] == species[None, :]).astype(jnp.float32)
    table = jnp.einsum(
        "sk,sa->ka",
        couplings.reshape(kinds, width * width),
        select,
        precision=lax.Precision.HIGHEST,
    )
    return table.reshape(width, width, species.shape[0])


def couple(totals, blocks):
    width = blocks.shape[0]
    atom_count = blocks.shape[2]
    folded = totals.reshape(totals.shape[0], width, atom_count)
    mixed = jnp.zeros_like(folded)
    for inner in range(width):
        mixed = mixed + folded[:, inner, None, :] * blocks[None, inner, :, :]
    return mixed.reshape(totals.shape[0], width * atom_count).astype(jnp.bfloat16)


def expand(coefs, projectors):
    return jnp.einsum("bp,gp->bg", coefs, projectors, preferred_element_type=jnp.float32).astype(
        jnp.bfloat16
    )


def on_device(orbitals, local_part, projectors, couplings, species):
    blocks = select_blocks(couplings, species)
    slab_orbitals = lax.all_to_all(
        orbitals, ("band", "ga"), split_axis=1, concat_axis=0, tiled=True
    )
    partial_value = jnp.dot(slab_orbitals, projectors, preferred_element_type=jnp.float32)
    devices = lax.axis_size(("band", "ga"))
    pieces = lax.all_to_all(
        partial_value.astype(jnp.bfloat16), ("band", "ga"), split_axis=0, concat_axis=0, tiled=True
    )
    pieces = pieces.reshape(devices, pieces.shape[0] // devices, pieces.shape[1])
    totals = jnp.sum(pieces.astype(jnp.float32), axis=0)
    coefs = lax.all_gather(couple(totals, blocks), ("band", "ga"), axis=0, tiled=True)
    slab_correction = expand(coefs, projectors)
    correction = lax.all_to_all(
        slab_correction, ("band", "ga"), split_axis=0, concat_axis=1, tiled=True
    )
    correction = lax.optimization_barrier(correction)
    return (local_part.astype(jnp.float32) + correction.astype(jnp.float32)).astype(jnp.bfloat16)


def solution(mesh):
    placed = (P(("band", "ga"), None), P(("band", "ga"), None), P(("band", "ga"), None), P(), P())
    return jax.shard_map(
        on_device, mesh=mesh, in_specs=placed, out_specs=P(("band", "ga"), None), check_vma=False
    )
```
